256 devices in a mesh: grp: 2 (over z), row: 128 (over y, x, core).
Axes of the slice: x: 8, y: 8, z: 2, core: 2. Of those that a mesh axis runs over, the one named last changes fastest.
The devices are a block of a 8x8x16 slice.
Arguments:
- concentration: float32 [16, 1024, 1024], P('grp', 'row'), parts along dimension 0, may hold values from -0.95 to 1.35
- target_mass: float32 [16], P('grp'), parts along dimension 0, may hold values from 0 to 0.4
- mobility: float32 [16], P('grp'), parts along dimension 0, may hold values from 0.5 to 2
Outputs:
- updated: float32 [16, 1024, 1024], P('grp', 'row'), parts along dimension 0
- residual: float32 [16], P('grp'), parts along dimension 0
The draws below stay inside these ranges and needn't reach their ends.
There are 2 independent parts, one for each index of `grp`. The reference program is written for one: setup_inputs(seed, part) draws one part's arguments, and reference() takes and returns one part's arrays. A program takes and returns all parts, laid end to end along the dimension named above; each array names one. Nothing has to cross between parts.
All inputs are finite; a program needn't handle non-finite values.
Results may differ from the reference program's by a relative error of at most 0.00005.
Values sent between devices are 32-bit elements; how exact they have to be, the bound alone decides.
A program may use at most 64 MiB of HBM per device.

```python
import math
import jax
import jax.numpy as jnp
from jax import lax

NX = 1024
NY = 1024
PLANES = 8


def draw_concentration(key, part):
    random_key = jax.random.fold_in(key, 17)
    position = jnp.arange(NX, dtype=jnp.float32) / (NX - 1)
    profile = 0.1 + 0.2 * position
    jitter = 0.35 * jax.random.truncated_normal(random_key, -3.0, 3.0, (PLANES, NX, NY), jnp.float32)
    return profile[None, :, None] + jitter


def setup_inputs(seed: int = 0, part: int = 0) -> dict:
    key_list = jax.random.split(jax.random.key(seed), 4)
    own_keys = jax.random.split(jax.random.fold_in(key_list[3], part), 4)
    concentration = draw_concentration(jax.random.fold_in(jax.random.fold_in(key_list[3], part), 71), part)
    target_mass = jnp.clip(jax.random.uniform(own_keys[1], (PLANES,), jnp.float32, 0.0, 0.4), 0.0, 0.4)
    mobility = jnp.clip(jnp.exp(jax.random.uniform(own_keys[2], (PLANES,), jnp.float32, math.log(0.5), math.log(2.0))), 0.5, 2.0)
    return dict(concentration=concentration, target_mass=target_mass, mobility=mobility)


stiffness = 1.0
time_step = 0.05
stabilizer = 2.0


def spectral_axis(length):
    position = jnp.arange(length, dtype=jnp.int32)
    signed = jnp.where(position < length // 2, position, position - length)
    angular = signed.astype(jnp.float32) * (2.0 * math.pi / length)
    derivative = jnp.where(position == length // 2, jnp.float32(0.0), angular)
    return angular, derivative


def one_plane(inputs):
    phase_field, target, scale = inputs
    angular_x, derivative_x = spectral_axis(NX)
    angular_y, derivative_y = spectral_axis(NY)
    square = angular_x[:, None] ** 2 + angular_y[None, :] ** 2
    slope_rows = derivative_x[:, None]
    slope_cols = derivative_y[None, :]
    field_hat = jnp.fft.fft2(phase_field)
    cubic_hat = jnp.fft.fft2(phase_field * phase_field * phase_field - phase_field)
    chem_hat = cubic_hat + stiffness * square * field_hat
    grad_rows = jnp.real(jnp.fft.ifft2(1j * slope_rows * chem_hat))
    grad_cols = jnp.real(jnp.fft.ifft2(1j * slope_cols * chem_hat))
    weight = scale / (1.0 + phase_field * phase_field)
    flux_rows = jnp.fft.fft2(weight * grad_rows)
    flux_cols = jnp.fft.fft2(weight * grad_cols)
    div_hat = 1j * slope_rows * flux_rows + 1j * slope_cols * flux_cols
    denom = 1.0 + time_step * scale * (stabilizer * square + stiffness * square * square)
    fresh = phase_field + jnp.real(jnp.fft.ifft2(time_step * div_hat / denom))
    residual = jnp.mean(fresh) - target
    return fresh - residual, residual


def reference(concentration, target_mass, mobility):
    updated, residual = lax.map(one_plane, (concentration, target_mass, mobility))
    return updated, residual
```

```python
import functools
import math

import jax
import jax.numpy as jnp
import ml_dtypes
import numpy as np
from jax import lax
from jax.experimental import pallas as pl
from jax.experimental.pallas import tpu as pltpu
from jax.sharding import Mesh
from jax.sharding import PartitionSpec as P

ROW = ("row_0", "row_1", "row_2")
MESH = pl.DeviceIdType.MESH
SIDE = (8, 8, 2)
PEERS = SIDE[0] * SIDE[1] * SIDE[2]
LANES = 128
CHUNKS = 1

stiffness = 1.0
time_step = 0.05
stabilizer = 2.0


def split(table):
    high = table.astype(ml_dtypes.bfloat16)
    low = (table - high.astype(np.float64)).astype(ml_dtypes.bfloat16)
    return np.stack([high, low])


def circulants(length):
    position = np.arange(length)
    signed = np.where(position < length // 2, position, position - length)
    angular = signed * (2.0 * math.pi / length)
    derivative = np.where(position == length // 2, 0.0, angular)
    offset = (position[None, :] - position[:, None]) % length
    second = np.fft.ifft(angular**2).real[offset]
    first = np.fft.ifft(1j * derivative).real[offset]
    return second, first


def real_basis(length):
    wave, is_sine = slots(np.arange(length), length)
    angle = np.outer(np.arange(length), wave) % length * (2.0 * math.pi / length)
    plain = (wave == 0) | (wave == length // 2)
    scale = np.where(plain, np.sqrt(1.0 / length), np.sqrt(2.0 / length))
    return np.where(is_sine & ~plain, np.sin(angle), np.cos(angle)) * scale


def slots(slot, length):
    quarter = length // 4
    odd = slot // (2 * quarter)
    within = slot % (2 * quarter)
    is_sine = within // quarter
    wave = 2 * (within % quarter) + odd
    nyquist = (is_sine == 1) & (wave == 0)
    if isinstance(slot, np.ndarray):
        return np.where(nyquist, length // 2, wave), is_sine == 1
    return jnp.where(nyquist, length // 2, wave), is_sine == 1


def row_tiles(matrix):
    return np.stack([matrix[:256, d * 256 : (d + 1) * 256] for d in range(matrix.shape[0] // 256)])


def column_tiles(matrix, order):
    permuted = matrix[order][:, order]
    blocks = permuted.shape[0] // 256
    out = []
    for d in range(1 - blocks, blocks):
        i, j = max(0, -d), max(0, d)
        out.append(permuted[i * 256 : (i + 1) * 256, j * 256 : (j + 1) * 256])
    return np.stack(out)


@functools.cache
def tables(length, rows_local):
    second, first = circulants(length)
    basis = real_basis(length)
    half = length // 2
    order = np.arange(length).reshape(length // rows_local, rows_local).T.reshape(-1)
    halves = np.stack([basis[:half, :half], basis[:half, half:]])
    back = np.swapaxes(halves, 1, 2)
    return tuple(
        split(t)
        for t in (
            row_tiles(second),
            column_tiles(second, order),
            column_tiles(first, order),
            row_tiles(first),
            halves,
            basis[order],
            basis[order].T,
            back,
        )
    )


def parts(x):
    high = x.astype(jnp.bfloat16)
    low = (x - high.astype(jnp.float32)).astype(jnp.bfloat16)
    return high, jnp.concatenate([high, low], axis=0)


def product(x, pieces):
    m = x.shape[0]
    high, both = parts(x)
    inputs, outputs, piece = pieces
    out = []
    for j in range(outputs):
        total = None
        for i in range(inputs):
            at = slice(i * 256, (i + 1) * 256)
            wide = jnp.dot(both[:, at], piece(i, j, 0), preferred_element_type=jnp.float32)
            narrow = jnp.dot(high[:, at], piece(i, j, 1), preferred_element_type=jnp.float32)
            term = (wide, narrow)
            total = term if total is None else (total[0] + wide, total[1] + narrow)
        out.append(total[0][:m] + total[0][m:] + total[1])
    return jnp.concatenate(out, axis=1)


def by_row(ref):
    n = ref.shape[1]
    return n, n, lambda i, j, part: ref[part, (j - i) % n]


def by_column(ref):
    n = (ref.shape[1] + 1) // 2
    return n, n, lambda i, j, part: ref[part, j - i + n - 1]


def dense(ref):
    n = ref.shape[1] // 256
    return n, n, lambda i, j, part: ref[part, i * 256 : (i + 1) * 256, j * 256 : (j + 1) * 256]


def dense_half(ref, which):
    n = ref.shape[2] // 256
    return n, n, lambda i, j, part: ref[part, which, i * 256 : (i + 1) * 256, j * 256 : (j + 1) * 256]


def kernel(
    x_ref, target_ref, mobility_ref,
    t0, t1, t2, t3, t4, t5, t6, t7,
    out_ref, residual_ref,
    v0, v1, v2, v3, v4, v5, v6, v7,
    send1, take1, send2, take2, send3, take3, send4, take4,
    turn, held, sum_mine, sum_row, sum_total, sum_all,
    table_sem, send_sem, take_sem, sum_send, sum_take,
):
    planes, rows_local, width = x_ref.shape
    ncs = CHUNKS
    each = planes // ncs
    hbm_tables = (t0, t1, t2, t3, t4, t5, t6, t7)
    vmem_tables = (v0, v1, v2, v3, v4, v5, v6, v7)
    y, x, c = (lax.axis_index(a) for a in ROW)
    me = (y * SIDE[1] + x) * SIDE[2] + c

    def place(dy, dx, dc):
        return (y + dy) & (SIDE[0] - 1), (x + dx) & (SIDE[1] - 1), (c + dc) & (SIDE[2] - 1)

    def device(p):
        return dict(zip(ROW, p, strict=True))

    def far_first(t):
        half = (t + 1) >> 1
        return 4 + half - 2 * half * (t & 1)

    def for_peers(act):
        def turn_of(k, _):
            for i in range(8):
                dy = (4, 3, 5, 2, 6, 1, 7, 0)[i]
                dx = far_first((k + i) & 7)
                for dc in range(2):
                    if i == 7 and dc == 0:
                        pl.when(k != 0)(functools.partial(act, place(dy, dx, dc)))
                    else:
                        act(place(dy, dx, dc))
            return 0

        lax.fori_loop(0, 8, turn_of, 0)

    barrier = pltpu.get_barrier_semaphore()

    def greet(p):
        pl.semaphore_signal(barrier, inc=1, device_id=device(p), device_id_type=MESH)

    for_peers(greet)
    loads = [
        pltpu.make_async_copy(h, v, table_sem.at[i])
        for i, (h, v) in enumerate(zip(hbm_tables, vmem_tables, strict=True))
    ]
    for load in loads:
        load.start()

    def start_exchange(src, dst, n, phase):
        rows = src.shape[1] // PEERS

        def send(p):
            to = (p[0] * SIDE[1] + p[1]) * SIDE[2] + p[2]
            pltpu.make_async_remote_copy(
                src_ref=src.at[n, pl.ds(pl.multiple_of(to * rows, rows), rows)],
                dst_ref=dst.at[n, pl.ds(pl.multiple_of(me * rows, rows), rows)],
                send_sem=send_sem.at[n, phase],
                recv_sem=take_sem.at[n, phase],
                device_id=device(p),
                device_id_type=MESH,
            ).start()

        for_peers(send)
        own = pl.ds(pl.multiple_of(me * rows, rows), rows)
        dst[n, own, :] = src[n, own, :]

    def whole(src, dst, n, phase):
        rows = src.shape[1] // PEERS
        return pltpu.make_async_remote_copy(
            src_ref=src.at[n, pl.ds(0, rows * (PEERS - 1))],
            dst_ref=dst.at[n, pl.ds(0, rows * (PEERS - 1))],
            send_sem=send_sem.at[n, phase],
            recv_sem=take_sem.at[n, phase],
            device_id=device((y, x, c)),
            device_id_type=MESH,
        )

    def pack_rows(fields, dst, n):
        shares = 16 // len(fields) // each
        wide = width // shares
        for j in range(wide // LANES):
            block = [
                f[:, s * wide + j * LANES : s * wide + (j + 1) * LANES] for f in fields for s in range(shares)
            ]
            dst[n, j * LANES : (j + 1) * LANES, :] = jnp.concatenate(block, axis=0).T

    def unpack_rows(src, n, count):
        shares = 16 // count // each
        wide = width // shares
        rows = each * rows_local
        got = [src[n, j * LANES : (j + 1) * LANES, :].T for j in range(wide // LANES)]
        return [
            jnp.concatenate(
                [g[(f * shares + s) * rows : (f * shares + s + 1) * rows] for s in range(shares) for g in got], axis=1
            )
            for f in range(count)
        ]

    def unpack_columns(src, n, count):
        deep = src.shape[1] // PEERS
        for s in range(deep):
            turn[s * LANES : (s + 1) * LANES, :] = src[n, pl.ds(s, PEERS, stride=deep), :].T
        out = [[] for _ in range(count)]
        for a in range(rows_local):
            got = turn[pl.ds(a, deep * 16, stride=rows_local), :].reshape(deep, count, 16 // count, LANES)
            for f in range(count):
                out[f].append(got[:, f].reshape(deep * 16 // count, LANES))
        return [jnp.concatenate(o, axis=1) for o in out]

    def pack_columns(fields, dst, n):
        count = len(fields)
        deep = dst.shape[1] // PEERS
        for a in range(rows_local):
            got = [f[:, a * LANES : (a + 1) * LANES].reshape(deep, 1, 16 // count, LANES) for f in fields]
            turn[pl.ds(a, deep * 16, stride=rows_local), :] = jnp.concatenate(got, axis=1).reshape(deep * 16, LANES)
        for s in range(deep):
            dst[n, pl.ds(s, PEERS, stride=deep), :] = turn[s * LANES : (s + 1) * LANES, :].T

    def per_plane(shape, plane_of_row, first_plane):
        out = jnp.zeros(shape, jnp.float32)
        for p in range(each):
            out = jnp.where(plane_of_row == p, mobility_ref[first_plane + p], out)
        return out

    def ready(i):
        loads[i].wait()
        return vmem_tables[i]

    waited = set()

    def table(i):
        if i not in waited:
            waited.add(i)
            loads[i].wait()
        return vmem_tables[i]

    def start_rows(n):
        field = x_ref[n * each : (n + 1) * each].reshape(each * rows_local, width)
        local = field * field * field - field + stiffness * product(field, by_row(table(0)))
        held[n] = local
        pack_rows([field, local], send1, n)

    def columns_middle(n):
        field, local = unpack_columns(take1, n, 2)
        potential = local + stiffness * product(field, by_column(table(1)))
        slope = product(potential, by_column(table(2)))
        rows = lax.broadcasted_iota(jnp.int32, (field.shape[0], LANES), 0)
        scale = per_plane(rows.shape, rows % each, n * each)
        scale = jnp.concatenate([scale] * (field.shape[1] // LANES), axis=1)
        weight = scale / (1.0 + field * field)
        pack_columns([potential, product(weight * slope, by_column(table(2)))], send2, n)

    def rows_middle(n):
        potential, spread = unpack_rows(take2, n, 2)
        slope = product(potential, by_row(table(3)))
        field = x_ref[n * each : (n + 1) * each].reshape(each * rows_local, width)
        rows = lax.broadcasted_iota(jnp.int32, (field.shape[0], LANES), 0)
        scale = per_plane(rows.shape, rows // rows_local, n * each)
        scale = jnp.concatenate([scale] * (width // LANES), axis=1)
        weight = scale / (1.0 + field * field)
        total = spread + product(weight * slope, by_row(table(3)))
        first, last = total[:, : width // 2], total[:, width // 2 :]
        basis = table(4)
        spectrum = jnp.concatenate(
            [product(first + last, dense_half(basis, 0)), product(first - last, dense_half(basis, 1))], axis=1
        )
        pack_rows([spectrum], send3, n)

    def columns_solve(n):
        deep = take3.shape[1] // PEERS
        shares = 16 // each
        rows = lax.broadcasted_iota(jnp.int32, (deep * 16, LANES), 0)
        slot_y = (rows % 16) // each * (width // shares) + me * deep + rows // 16
        scale = per_plane(rows.shape, rows % each, n * each)
        step = 2.0 * math.pi / width
        wave_y = slots(slot_y, width)[0].astype(jnp.float32) * step
        length = PEERS * rows_local
        slot_x = lax.broadcasted_iota(jnp.int32, (8, length), 1)
        wave_x = slots(slot_x, length)[0].astype(jnp.float32) * (2.0 * math.pi / length)
        square_x = (wave_x * wave_x)[:1]
        wide = length // LANES
        square = jnp.concatenate([wave_y * wave_y] * wide, axis=1) + square_x
        denom = 1.0 + time_step * jnp.concatenate([scale] * wide, axis=1) * (
            stabilizer * square + stiffness * square * square
        )
        factor = time_step / denom
        whole(send3, take3, n, 2).wait_recv()
        (spectrum,) = unpack_columns(take3, n, 1)
        solved = product(spectrum, dense(table(5))) * factor
        pack_columns([product(solved, dense(table(6)))], send4, n)

    def residual():
        total = jnp.sum(sum_all[...], axis=0)
        length = PEERS * rows_local
        mean = jnp.sum(total, axis=1, keepdims=True) * (1.0 / (length * width))
        row = lax.broadcasted_iota(jnp.int32, (planes, LANES), 0)
        target = jnp.zeros((planes, LANES), jnp.float32)
        for p in range(planes):
            target = jnp.where(row == p, target_ref[p], target)
        residual_ref[...] = mean - target

    def rows_end(n):
        (spectrum,) = unpack_rows(take4, n, 1)
        back = table(7)
        even = product(spectrum[:, : width // 2], dense_half(back, 0))
        odd = product(spectrum[:, width // 2 :], dense_half(back, 1))
        change = jnp.concatenate([even + odd, even - odd], axis=1).reshape(each, rows_local, width)
        shift = residual_ref[n * each : (n + 1) * each, :][:, None, :]
        shift = jnp.concatenate([shift] * (width // LANES), axis=2)
        out_ref[n * each : (n + 1) * each] = x_ref[n * each : (n + 1) * each] + change - shift

    def sum_slot(stage, p):
        return p[0] if stage else p[1] * SIDE[2] + p[2]

    def sum_copy(stage, index, p, sender):
        src, dst = ((sum_mine, sum_row), (sum_total, sum_all))[stage]
        slot = sum_slot(stage, sender)
        return pltpu.make_async_remote_copy(
            src_ref=src, dst_ref=dst.at[slot], send_sem=sum_send.at[stage, index], recv_sem=sum_take.at[stage, slot],
            device_id=device(p), device_id_type=MESH,
        )

    def start_sums(stage, places):
        for i, d in enumerate(places):
            sum_copy(stage, i, place(*d), (y, x, c)).start()
        src, dst = ((sum_mine, sum_row), (sum_total, sum_all))[stage]
        dst[sum_slot(stage, (y, x, c))] = src[...]

    def take_sums(stage, places):
        for i, d in enumerate(places):
            sum_copy(stage, i, (y, x, c), place(*d)).wait_recv()

    near = [(0, dx, dc) for dx in range(SIDE[1]) for dc in range(SIDE[2])][1:]
    across = [(dy, 0, 0) for dy in range(1, SIDE[0])]

    for n in range(ncs):
        start_rows(n)
    summed = jnp.sum(x_ref[...], axis=1)
    part = summed[:, :LANES]
    for j in range(1, width // LANES):
        part = part + summed[:, j * LANES : (j + 1) * LANES]
    sum_mine[...] = part

    pl.semaphore_wait(barrier, PEERS - 1)
    for n in range(ncs):
        start_exchange(send1, take1, n, 0)
    start_sums(0, near)
    for n in range(ncs):
        whole(send1, take1, n, 0).wait_recv()
        columns_middle(n)
        start_exchange(send2, take2, n, 1)
    take_sums(0, near)
    sum_total[...] = jnp.sum(sum_row[...], axis=0)
    start_sums(1, across)
    for n in range(ncs):
        whole(send2, take2, n, 1).wait_recv()
        rows_middle(n)
        start_exchange(send3, take3, n, 2)
    take_sums(1, across)
    residual()
    for n in range(ncs):
        columns_solve(n)
        start_exchange(send4, take4, n, 3)
    for n in range(ncs):
        whole(send4, take4, n, 3).wait_recv()
        rows_end(n)
    for n in range(ncs):
        for phase, (src, dst) in enumerate(((send1, take1), (send2, take2), (send3, take3), (send4, take4))):
            whole(src, dst, n, phase).wait_send()
    for stage, places in enumerate((near, across)):
        for i, d in enumerate(places):
            sum_copy(stage, i, place(*d), (y, x, c)).wait_send()


def local(concentration, target_mass, mobility):
    planes, rows_local, width = concentration.shape
    data = tables(width, rows_local)
    ncs = CHUNKS
    two = pltpu.VMEM((ncs, PEERS * planes // ncs, LANES), jnp.float32)
    one = pltpu.VMEM((ncs, PEERS * planes // ncs // 2, LANES), jnp.float32)
    vmem = pl.BlockSpec(memory_space=pltpu.VMEM)
    smem = pl.BlockSpec(memory_space=pltpu.SMEM)
    updated, residual = pl.pallas_call(
        kernel,
        out_shape=(
            jax.ShapeDtypeStruct(concentration.shape, jnp.float32),
            jax.ShapeDtypeStruct((planes, LANES), jnp.float32),
        ),
        in_specs=[vmem, smem, smem] + [pl.BlockSpec(memory_space=pl.ANY)] * len(data),
        out_specs=(vmem, vmem),
        scratch_shapes=[pltpu.VMEM(t.shape, jnp.bfloat16) for t in data]
        + [two] * 4
        + [one] * 4
        + [
            pltpu.VMEM((PEERS * planes // ncs, LANES), jnp.float32),
            pltpu.VMEM((ncs, planes // ncs * rows_local, width), jnp.float32),
            pltpu.VMEM((planes, LANES), jnp.float32),
            pltpu.VMEM((SIDE[1] * SIDE[2], planes, LANES), jnp.float32),
            pltpu.VMEM((planes, LANES), jnp.float32),
            pltpu.VMEM((SIDE[0], planes, LANES), jnp.float32),
            pltpu.SemaphoreType.DMA((len(data),)),
            pltpu.SemaphoreType.DMA((ncs, 4)),
            pltpu.SemaphoreType.DMA((ncs, 4)),
            pltpu.SemaphoreType.DMA((2, SIDE[1] * SIDE[2])),
            pltpu.SemaphoreType.DMA((2, SIDE[1] * SIDE[2])),
        ],
        compiler_params=pltpu.CompilerParams(
            collective_id=0, has_side_effects=True, vmem_limit_bytes=60 * 2**20
        ),
    )(concentration, target_mass, mobility, *[jnp.asarray(t) for t in data])
    return updated, residual[:, 0]


def solution(mesh):
    torus = Mesh(mesh.devices.reshape(mesh.shape["grp"], *SIDE), ("grp", *ROW))
    in_specs = (P("grp", ROW, None), P("grp"), P("grp"))
    out_specs = (P("grp", ROW, None), P("grp"))
    return jax.shard_map(local, mesh=torus, in_specs=in_specs, out_specs=out_specs, check_vma=False)
```

```python
import functools
import math

import jax
import jax.numpy as jnp
import ml_dtypes
import numpy as np
from jax import lax
from jax.experimental import pallas as pl
from jax.experimental.pallas import tpu as pltpu
from jax.sharding import Mesh
from jax.sharding import PartitionSpec as P

ROW = ("row_0", "row_1", "row_2")
MESH = pl.DeviceIdType.MESH
SIDE = (8, 8, 2)
CHIPS = SIDE[0] * SIDE[1]
CORES = SIDE[2]
LANES = 128
CHUNKS = 2

stiffness = 1.0
time_step = 0.05
stabilizer = 2.0


def split(table):
    high = table.astype(ml_dtypes.bfloat16)
    low = (table - high.astype(np.float64)).astype(ml_dtypes.bfloat16)
    return np.stack([high, low])


def circulants(length):
    position = np.arange(length)
    signed = np.where(position < length // 2, position, position - length)
    angular = signed * (2.0 * math.pi / length)
    derivative = np.where(position == length // 2, 0.0, angular)
    offset = (position[None, :] - position[:, None]) % length
    second = np.fft.ifft(angular**2).real[offset]
    first = np.fft.ifft(1j * derivative).real[offset]
    return second, first


def real_basis(length):
    wave, is_sine = slots(np.arange(length), length)
    angle = np.outer(np.arange(length), wave) % length * (2.0 * math.pi / length)
    plain = (wave == 0) | (wave == length // 2)
    scale = np.where(plain, np.sqrt(1.0 / length), np.sqrt(2.0 / length))
    return np.where(is_sine & ~plain, np.sin(angle), np.cos(angle)) * scale


def slots(slot, length):
    quarter = length // 4
    odd = slot // (2 * quarter)
    within = slot % (2 * quarter)
    is_sine = within // quarter
    wave = 2 * (within % quarter) + odd
    nyquist = (is_sine == 1) & (wave == 0)
    if isinstance(slot, np.ndarray):
        return np.where(nyquist, length // 2, wave), is_sine == 1
    return jnp.where(nyquist, length // 2, wave), is_sine == 1


def halves(matrix, order):
    half = matrix.shape[0] // 2
    near, far = matrix[order][:, order], matrix[order][:, order + half]
    return np.stack([near + far, near - far]) / 2


@functools.cache
def tables(length):
    second, first = circulants(length)
    basis = real_basis(length)
    half = length // 2
    rows = np.arange(half)
    columns = rows.reshape(CHIPS // 2, CORES, -1).transpose(2, 1, 0).reshape(-1)
    row_basis, column_basis = (np.stack([basis[o][:, :half], basis[o][:, half:]]) for o in (rows, columns))
    return tuple(
        split(t)
        for t in (
            halves(second, rows),
            halves(second, columns),
            halves(first, columns),
            halves(first, rows),
            row_basis,
            column_basis,
            np.swapaxes(column_basis, 1, 2),
            np.swapaxes(row_basis, 1, 2),
        )
    )


def parts(x):
    high = x.astype(jnp.bfloat16)
    low = (x - high.astype(jnp.float32)).astype(jnp.bfloat16)
    return high, jnp.concatenate([high, low], axis=0)


def product(x, pieces):
    m = x.shape[0]
    high, both = parts(x)
    inputs, outputs, piece = pieces
    out = []
    for j in range(outputs):
        total = None
        for i in range(inputs):
            at = slice(i * 256, (i + 1) * 256)
            wide = jnp.dot(both[:, at], piece(i, j, 0), preferred_element_type=jnp.float32)
            narrow = jnp.dot(high[:, at], piece(i, j, 1), preferred_element_type=jnp.float32)
            term = (wide, narrow)
            total = term if total is None else (total[0] + wide, total[1] + narrow)
        out.append(total[0][:m] + total[0][m:] + total[1])
    return jnp.concatenate(out, axis=1)


def table_pieces(ref, which):
    n = ref.shape[2] // 256
    return n, n, lambda i, j, part: ref[part, which, i * 256 : (i + 1) * 256, j * 256 : (j + 1) * 256]


def analyse(x, ref):
    return product(x[0] + x[1], table_pieces(ref, 0)), product(x[0] - x[1], table_pieces(ref, 1))


def synthesise(z, ref):
    even, odd = product(z[0], table_pieces(ref, 0)), product(z[1], table_pieces(ref, 1))
    return even + odd, even - odd


def circulant(x, ref):
    even, odd = analyse(x, ref)
    return even + odd, even - odd


def cut(x):
    half = x.shape[1] // 2
    return x[:, :half], x[:, half:]


def join(x):
    return jnp.concatenate(x, axis=1)


def kernel(
    x_ref, target_hbm, mobility_hbm,
    t0, t1, t2, t3, t4, t5, t6, t7,
    out_ref, residual_ref,
    v0, v1, v2, v3, v4, v5, v6, v7,
    send1, take1, send2, take2, send3, take3, send4, take4,
    turn, mine, local_part, rows_of,
    sum0, sum1, take_sum0, take_sum1, target_ref, mobility_ref,
    load_sem, send_sem, take_sem, swap_send, swap_take, sum_send, sum_take,
):
    planes, rows_local, width = x_ref.shape
    ncs = CHUNKS
    own = planes // CORES
    each = own // ncs
    vmem_tables = (v0, v1, v2, v3, v4, v5, v6, v7)
    y, x, c = (lax.axis_index(a) for a in ROW)
    chip = y * SIDE[1] + x
    other = 1 - c

    def device(p):
        return dict(zip(ROW, p, strict=True))

    def far_first(t):
        half = (t + 1) >> 1
        return 4 + half - 2 * half * (t & 1)

    def for_chips(act):
        def turn_of(k, _):
            for i in range(8):
                to_y = (y + (4, 3, 5, 2, 6, 1, 7, 0)[i]) & (SIDE[0] - 1)
                to_x = (x + far_first((k + i) & 7)) & (SIDE[1] - 1)
                if i == 7:
                    pl.when(k != 0)(functools.partial(act, to_y, to_x))
                else:
                    act(to_y, to_x)
            return 0

        lax.fori_loop(0, 8, turn_of, 0)

    first_loads = [
        pltpu.make_async_copy(a, b, load_sem.at[i])
        for i, (a, b) in enumerate(((x_ref, mine), (mobility_hbm, mobility_ref), (target_hbm, target_ref)))
    ]
    loads = [
        pltpu.make_async_copy(h, v, load_sem.at[3 + i])
        for i, (h, v) in enumerate(zip((t0, t1, t2, t3, t4, t5, t6, t7), vmem_tables, strict=True))
    ]
    for load in (first_loads[0], loads[0], *first_loads[1:]):
        load.start()

    barrier = pltpu.get_barrier_semaphore()

    def greet(to_y, to_x):
        for core in range(CORES):
            pl.semaphore_signal(barrier, inc=1, device_id=device((to_y, to_x, core)), device_id_type=MESH)

    for_chips(greet)
    pl.semaphore_signal(barrier, inc=1, device_id=device((y, x, other)), device_id_type=MESH)
    for load in loads[1:]:
        load.start()

    def spot(core, position, deep):
        return pl.ds(pl.multiple_of((core * CHIPS + position) * deep, deep), deep)

    def copy_out(src_ref, dst_ref, n, phase, p):
        return pltpu.make_async_remote_copy(
            src_ref=src_ref, dst_ref=dst_ref, send_sem=send_sem.at[n, phase], recv_sem=take_sem.at[n, phase],
            device_id=device(p), device_id_type=MESH,
        )

    def start_to_cores(src, dst, n, phase):
        deep = src.shape[1] // CHIPS // CORES
        here = spot(c, chip, deep)

        def send_one(to_y, to_x, core):
            there = spot(core, to_y * SIDE[1] + to_x, deep)
            copy_out(src.at[n, there], dst.at[n, here], n, phase, (to_y, to_x, core)).start()

        def send(to_y, to_x):
            for core in range(CORES):
                send_one(to_y, to_x, core)

        for_chips(send)
        send_one(y, x, other)
        dst[n, here, :] = src[n, here, :]

    def start_to_chips(src, dst, n, phase):
        deep = src.shape[2] // CHIPS
        here = spot(0, chip, deep)

        def send(to_y, to_x):
            there = spot(0, to_y * SIDE[1] + to_x, deep)
            copy_out(src.at[n, :, there], dst.at[n, :, here], n, phase, (to_y, to_x, c)).start()

        for_chips(send)
        for core in range(CORES):
            dst[n, core, here, :] = src[n, core, here, :]

    def whole(src, dst, n, phase):
        if len(src.shape) == 3:
            deep = src.shape[1] // CHIPS // CORES
            at = (n, pl.ds(0, deep * (CHIPS * CORES - 1)))
        else:
            deep = src.shape[2] // CHIPS
            at = (n, slice(None), pl.ds(0, deep * (CHIPS - 1)))
        return copy_out(src.at[at], dst.at[at], n, phase, (y, x, other))

    def part(ref, n, core):
        if len(ref.shape) == 3:
            rows = ref.shape[1] // CORES
            return ref.at[n, pl.ds(core * rows, rows)], rows // CHIPS
        return ref.at[n, core], ref.shape[2] // CHIPS

    def swap(n):
        return pltpu.make_async_remote_copy(
            src_ref=mine.at[pl.ds(other * own + n * each, each)],
            dst_ref=rows_of.at[n, c],
            send_sem=swap_send.at[n],
            recv_sem=swap_take.at[n],
            device_id=device((y, x, other)),
            device_id_type=MESH,
        )

    def pack_rows(fields, dst, n, core):
        dst, _ = part(dst, n, core)
        shares = 16 // len(fields) // each
        wide = width // shares
        for j in range(wide // LANES):
            block = [
                f[:, s * wide + j * LANES : s * wide + (j + 1) * LANES] for f in fields for s in range(shares)
            ]
            dst[j * LANES : (j + 1) * LANES, :] = jnp.concatenate(block, axis=0).T

    def unpack_rows(src, n, count):
        shares = 16 // count // each
        wide = width // shares
        rows = each * rows_local
        out = [[] for _ in range(count)]
        for core in range(CORES):
            ref, _ = part(src, n, core)
            got = [ref[j * LANES : (j + 1) * LANES, :].T for j in range(wide // LANES)]
            for f in range(count):
                pieces = [g[(f * shares + s) * rows : (f * shares + s + 1) * rows] for s in range(shares) for g in got]
                out[f].append(jnp.concatenate(pieces, axis=1))
        return [jnp.concatenate(o, axis=0) for o in out]

    some = CHIPS // 2

    def low_half(rows):
        return lax.broadcasted_iota(jnp.int32, (rows, LANES), 1) < LANES // 2

    def unpack_columns(src, n, count):
        refs = [part(src, n, core) for core in range(CORES)]
        deep = refs[0][1]
        for s in range(deep):
            got = [
                ref[pl.ds(s + hi * some * deep, some, stride=deep), :] for hi in range(2) for ref, _ in refs
            ]
            turn[s * LANES : (s + 1) * LANES, :] = jnp.concatenate(got, axis=0).T
        out = [([], []) for _ in range(count)]
        low = low_half(deep * 16 // count)
        for a in range(0, rows_local, 2):
            pair = [
                turn[pl.ds(a + i, deep * 16, stride=rows_local), :].reshape(deep, count, 16 // count, LANES)
                for i in range(2)
            ]
            for f in range(count):
                one, two = (g[:, f].reshape(deep * 16 // count, LANES) for g in pair)
                out[f][0].append(jnp.where(low, one, pltpu.roll(two, LANES // 2, 1)))
                out[f][1].append(jnp.where(low, pltpu.roll(one, LANES // 2, 1), two))
        return [tuple(jnp.concatenate(h, axis=1) for h in o) for o in out]

    def pack_columns(fields, dst, n):
        count = len(fields)
        refs = [part(dst, n, core) for core in range(CORES)]
        deep = refs[0][1]
        low = low_half(deep * 16 // count)
        for a in range(0, rows_local, 2):
            at = slice(a // 2 * LANES, (a // 2 + 1) * LANES)
            pair = ([], [])
            for f in fields:
                near, far = f[0][:, at], f[1][:, at]
                pair[0].append(jnp.where(low, near, pltpu.roll(far, LANES // 2, 1)))
                pair[1].append(jnp.where(low, pltpu.roll(near, LANES // 2, 1), far))
            for i in range(2):
                got = [g.reshape(deep, 1, 16 // count, LANES) for g in pair[i]]
                turn[pl.ds(a + i, deep * 16, stride=rows_local), :] = jnp.concatenate(got, axis=1).reshape(
                    deep * 16, LANES
                )
        for s in range(deep):
            both = turn[s * LANES : (s + 1) * LANES, :].T
            for hi in range(2):
                for core, (ref, _) in enumerate(refs):
                    at = (hi * CORES + core) * some
                    ref[pl.ds(s + hi * some * deep, some, stride=deep), :] = both[at : at + some]

    def per_plane(shape, plane_of_row, n):
        out = jnp.zeros(shape, jnp.float32)
        for p in range(each):
            out = jnp.where(plane_of_row == p, mobility_ref[c * own + n * each + p], out)
        return out

    waited = set()

    def table(i):
        if i not in waited:
            waited.add(i)
            loads[i].wait()
        return vmem_tables[i]

    def start_fields():
        first_loads[0].wait()
        field = mine[...].reshape(planes * rows_local, width)
        local = field * field * field - field + stiffness * join(circulant(cut(field), table(0)))
        local_part[...] = local.reshape(planes, rows_local, width)
        for n in range(ncs):
            for core in range(CORES):
                at = slice(core * own + n * each, core * own + (n + 1) * each)
                fields = [ref[at].reshape(each * rows_local, width) for ref in (mine, local_part)]
                pack_rows(fields, send1, n, core)

    def columns_middle(n):
        field, local = unpack_columns(take1, n, 2)
        potential = [u + stiffness * v for u, v in zip(local, circulant(field, table(1)), strict=True)]
        slope = circulant(potential, table(2))
        rows = lax.broadcasted_iota(jnp.int32, (field[0].shape[0], LANES), 0)
        scale = per_plane(rows.shape, rows % each, n)
        scale = jnp.concatenate([scale] * (field[0].shape[1] // LANES), axis=1)
        flux = [scale / (1.0 + f * f) * g for f, g in zip(field, slope, strict=True)]
        pack_columns([potential, circulant(flux, table(2))], send2, n)

    def row_weight(n):
        for p in range(each):
            rows_of[n, c, p] = mine[c * own + n * each + p]
        swap(n).wait_recv()
        field = rows_of[n].reshape(CORES * each * rows_local, width)
        rows = lax.broadcasted_iota(jnp.int32, (field.shape[0], LANES), 0)
        scale = per_plane(rows.shape, rows // rows_local % each, n)
        scale = jnp.concatenate([scale] * (width // LANES), axis=1)
        rows_of[n] = (scale / (1.0 + field * field)).reshape(rows_of.shape[1:])

    def rows_middle(n):
        potential, spread = unpack_rows(take2, n, 2)
        slope = join(circulant(cut(potential), table(3)))
        weight = rows_of[n].reshape(slope.shape)
        total = spread + join(circulant(cut(weight * slope), table(3)))
        spectrum = join(analyse(cut(total), table(4)))
        rows = each * rows_local
        for core in range(CORES):
            pack_rows([spectrum[core * rows : (core + 1) * rows]], send3, n, core)

    def columns_solve(n):
        deep = take3.shape[2] // CHIPS
        shares = 16 // each
        rows = lax.broadcasted_iota(jnp.int32, (deep * 16, LANES), 0)
        slot_y = rows % 16 // each * (width // shares) + chip * deep + rows // 16
        scale = per_plane(rows.shape, rows % each, n)
        step = 2.0 * math.pi / width
        wave_y = slots(slot_y, width)[0].astype(jnp.float32) * step
        length = CHIPS * CORES * rows_local
        slot_x = lax.broadcasted_iota(jnp.int32, (8, length), 1)
        wave_x = slots(slot_x, length)[0].astype(jnp.float32) * (2.0 * math.pi / length)
        square_x = (wave_x * wave_x)[:1]
        wide = length // LANES
        square = jnp.concatenate([wave_y * wave_y] * wide, axis=1) + square_x
        denom = 1.0 + time_step * jnp.concatenate([scale] * wide, axis=1) * (
            stabilizer * square + stiffness * square * square
        )
        factor = time_step / denom
        whole(send3, take3, n, 2).wait_recv()
        (spectrum,) = unpack_columns(take3, n, 1)
        solved = [z * f for z, f in zip(analyse(spectrum, table(5)), cut(factor), strict=True)]
        pack_columns([synthesise(solved, table(6))], send4, n)

    def residual():
        total = jnp.sum(take_sum1[...], axis=0)
        length = CHIPS * CORES * rows_local
        mean = jnp.sum(total, axis=1, keepdims=True) * (1.0 / (length * width))
        row = lax.broadcasted_iota(jnp.int32, (planes, LANES), 0)
        first_loads[2].wait()
        target = jnp.zeros((planes, LANES), jnp.float32)
        for p in range(planes):
            target = jnp.where(row == p, target_ref[p], target)
        residual_ref[...] = mean - target

    def rows_end(n):
        (spectrum,) = unpack_rows(take4, n, 1)
        change = join(synthesise(cut(spectrum), table(7))).reshape(CORES, each, rows_local, width)
        for core in range(CORES):
            at = slice(core * own + n * each, core * own + (n + 1) * each)
            down = jnp.concatenate([residual_ref[at][:, None, :]] * (width // LANES), axis=2)
            out_ref[at] = mine[at] + change[core] - down

    sums = ((sum0, take_sum0), (sum1, take_sum1))
    near = [(0, dx, dc) for dx in range(SIDE[1]) for dc in range(SIDE[2])][1:]
    across = [(dy, 0, 0) for dy in range(1, SIDE[0])]

    def place(dy, dx, dc):
        return (y + dy) & (SIDE[0] - 1), (x + dx) & (SIDE[1] - 1), (c + dc) & (SIDE[2] - 1)

    def sum_slot(stage, p):
        return p[0] if stage else p[1] * SIDE[2] + p[2]

    def sum_copy(stage, index, p, sender):
        src, dst = sums[stage]
        slot = sum_slot(stage, sender)
        return pltpu.make_async_remote_copy(
            src_ref=src, dst_ref=dst.at[slot], send_sem=sum_send.at[stage, index], recv_sem=sum_take.at[stage, slot],
            device_id=device(p), device_id_type=MESH,
        )

    def start_sums(stage, places):
        for i, d in enumerate(places):
            sum_copy(stage, i, place(*d), (y, x, c)).start()
        src, dst = sums[stage]
        dst[sum_slot(stage, (y, x, c))] = src[...]

    def take_sums(stage, places):
        for i, d in enumerate(places):
            sum_copy(stage, i, (y, x, other), place(*d)).wait_recv()

    start_fields()
    summed = jnp.sum(mine[...], axis=1)
    partial = summed[:, :LANES]
    for j in range(1, width // LANES):
        partial = partial + summed[:, j * LANES : (j + 1) * LANES]
    sum0[...] = partial

    pl.semaphore_wait(barrier, CHIPS * CORES - 1)
    for n in range(ncs):
        start_to_cores(send1, take1, n, 0)
    start_sums(0, near)
    for n in range(ncs):
        swap(n).start()
    first_loads[1].wait()
    for n in range(ncs):
        row_weight(n)
    for n in range(ncs):
        whole(send1, take1, n, 0).wait_recv()
        columns_middle(n)
        start_to_chips(send2, take2, n, 1)
    take_sums(0, near)
    sum1[...] = jnp.sum(take_sum0[...], axis=0)
    start_sums(1, across)
    for n in range(ncs):
        whole(send2, take2, n, 1).wait_recv()
        rows_middle(n)
        start_to_chips(send3, take3, n, 2)
    for n in range(ncs):
        columns_solve(n)
        start_to_cores(send4, take4, n, 3)
    take_sums(1, across)
    residual()
    for n in range(ncs):
        whole(send4, take4, n, 3).wait_recv()
        rows_end(n)
    for n in range(ncs):
        for phase, (src, dst) in enumerate(((send1, take1), (send2, take2), (send3, take3), (send4, take4))):
            whole(src, dst, n, phase).wait_send()
        swap(n).wait_send()
    for stage, places in enumerate((near, across)):
        for i, d in enumerate(places):
            sum_copy(stage, i, place(*d), (y, x, c)).wait_send()


def hand_over(updated_ref, residual_ref, out_ref, out_residual_ref):
    out_ref[...] = updated_ref[...]
    for p in range(out_residual_ref.shape[0]):
        out_residual_ref[p] = residual_ref[p, 0]


def local(concentration, target_mass, mobility):
    planes, rows_local, width = concentration.shape
    data = tables(width)
    ncs = CHUNKS
    each = planes // CORES // ncs
    rows = CHIPS * CORES * each
    shape = {1: (ncs, 2 * rows, LANES), 2: (ncs, CORES, rows, LANES), 3: (ncs, CORES, rows // 2, LANES), 4: (ncs, rows, LANES)}
    vmem = pl.BlockSpec(memory_space=pltpu.VMEM)
    updated, residual = pl.pallas_call(
        kernel,
        out_shape=(
            jax.ShapeDtypeStruct(concentration.shape, jnp.float32),
            jax.ShapeDtypeStruct((planes, LANES), jnp.float32),
        ),
        in_specs=[pl.BlockSpec(memory_space=pl.ANY)] * (3 + len(data)),
        out_specs=(vmem, vmem),
        scratch_shapes=[pltpu.VMEM(t.shape, jnp.bfloat16) for t in data]
        + [pltpu.VMEM(shape[phase], jnp.float32) for phase in (1, 2, 3, 4) for _ in range(2)]
        + [
            pltpu.VMEM((2 * rows, LANES), jnp.float32),
            pltpu.VMEM((planes, rows_local, width), jnp.float32),
            pltpu.VMEM((planes, rows_local, width), jnp.float32),
            pltpu.VMEM((ncs, CORES, each, rows_local, width), jnp.float32),
            pltpu.VMEM((planes, LANES), jnp.float32),
            pltpu.VMEM((planes, LANES), jnp.float32),
            pltpu.VMEM((SIDE[1] * SIDE[2], planes, LANES), jnp.float32),
            pltpu.VMEM((SIDE[0], planes, LANES), jnp.float32),
            pltpu.SMEM((planes,), jnp.float32),
            pltpu.SMEM((planes,), jnp.float32),
            pltpu.SemaphoreType.DMA((3 + len(data),)),
            pltpu.SemaphoreType.DMA((ncs, 4)),
            pltpu.SemaphoreType.DMA((ncs, 4)),
            pltpu.SemaphoreType.DMA((ncs,)),
            pltpu.SemaphoreType.DMA((ncs,)),
            pltpu.SemaphoreType.DMA((2, SIDE[1] * SIDE[2])),
            pltpu.SemaphoreType.DMA((2, SIDE[1] * SIDE[2])),
        ],
        compiler_params=pltpu.CompilerParams(
            collective_id=0, has_side_effects=True, vmem_limit_bytes=30 * 2**20
        ),
    )(concentration, target_mass, mobility, *[jnp.asarray(t) for t in data])
    smem = pl.BlockSpec(memory_space=pltpu.SMEM)
    return pl.pallas_call(
        hand_over,
        out_shape=(
            jax.ShapeDtypeStruct(concentration.shape, jnp.float32),
            jax.ShapeDtypeStruct((planes,), jnp.float32),
        ),
        in_specs=[vmem, smem],
        out_specs=(vmem, smem),
    )(updated, residual)


def solution(mesh):
    torus = Mesh(mesh.devices.reshape(mesh.shape["grp"], *SIDE), ("grp", *ROW))
    in_specs = (P("grp", ROW, None), P("grp"), P("grp"))
    out_specs = (P("grp", ROW, None), P("grp"))
    return jax.shard_map(local, mesh=torus, in_specs=in_specs, out_specs=out_specs, check_vma=False)
```

```python
import functools
import math

import jax
import jax.numpy as jnp
import ml_dtypes
import numpy as np
from jax import lax
from jax.experimental import pallas as pl
from jax.experimental.pallas import tpu as pltpu
from jax.sharding import Mesh
from jax.sharding import PartitionSpec as P

ROW = ("row_0", "row_1", "row_2")
MESH = pl.DeviceIdType.MESH
SIDE = (8, 8, 2)
CHIPS = SIDE[0] * SIDE[1]
CORES = SIDE[2]
LANES = 128
CHUNKS = 2

stiffness = 1.0
time_step = 0.05
stabilizer = 2.0


def split(table):
    high = table.astype(ml_dtypes.bfloat16)
    low = (table - high.astype(np.float64)).astype(ml_dtypes.bfloat16)
    return np.stack([high, low])


def circulants(length):
    position = np.arange(length)
    signed = np.where(position < length // 2, position, position - length)
    angular = signed * (2.0 * math.pi / length)
    derivative = np.where(position == length // 2, 0.0, angular)
    offset = (position[None, :] - position[:, None]) % length
    second = np.fft.ifft(angular**2).real[offset]
    first = np.fft.ifft(1j * derivative).real[offset]
    return second, first


def real_basis(length):
    wave, is_sine = slots(np.arange(length), length)
    angle = np.outer(np.arange(length), wave) % length * (2.0 * math.pi / length)
    plain = (wave == 0) | (wave == length // 2)
    scale = np.where(plain, np.sqrt(1.0 / length), np.sqrt(2.0 / length))
    return np.where(is_sine & ~plain, np.sin(angle), np.cos(angle)) * scale


def slots(slot, length):
    quarter = length // 4
    odd = slot // (2 * quarter)
    within = slot % (2 * quarter)
    is_sine = within // quarter
    wave = 2 * (within % quarter) + odd
    nyquist = (is_sine == 1) & (wave == 0)
    if isinstance(slot, np.ndarray):
        return np.where(nyquist, length // 2, wave), is_sine == 1
    return jnp.where(nyquist, length // 2, wave), is_sine == 1


def halves(matrix, order):
    half = matrix.shape[0] // 2
    near, far = matrix[order][:, order], matrix[order][:, order + half]
    return np.stack([near + far, near - far]) / 2


@functools.cache
def tables(length):
    second, first = circulants(length)
    basis = real_basis(length)
    half = length // 2
    rows = np.arange(half)
    columns = rows.reshape(CHIPS // 2, CORES, -1).transpose(2, 1, 0).reshape(-1)
    row_basis, column_basis = (np.stack([basis[o][:, :half], basis[o][:, half:]]) for o in (rows, columns))
    return tuple(
        split(t)
        for t in (
            halves(second, rows),
            halves(second, columns),
            halves(first, columns),
            halves(first, rows),
            row_basis,
            column_basis,
            np.swapaxes(column_basis, 1, 2),
            np.swapaxes(row_basis, 1, 2),
        )
    )


def parts(x):
    high = x.astype(jnp.bfloat16)
    low = (x - high.astype(jnp.float32)).astype(jnp.bfloat16)
    return high, jnp.concatenate([high, low], axis=0)


def product(x, pieces):
    m = x.shape[0]
    high, both = parts(x)
    inputs, outputs, piece = pieces
    out = []
    for j in range(outputs):
        total = None
        for i in range(inputs):
            at = slice(i * 256, (i + 1) * 256)
            wide = jnp.dot(both[:, at], piece(i, j, 0), preferred_element_type=jnp.float32)
            narrow = jnp.dot(high[:, at], piece(i, j, 1), preferred_element_type=jnp.float32)
            term = (wide, narrow)
            total = term if total is None else (total[0] + wide, total[1] + narrow)
        out.append(total[0][:m] + total[0][m:] + total[1])
    return jnp.concatenate(out, axis=1)


def table_pieces(ref, which):
    n = ref.shape[2] // 256
    return n, n, lambda i, j, part: ref[part, which, i * 256 : (i + 1) * 256, j * 256 : (j + 1) * 256]


def analyse(x, ref):
    return product(x[0] + x[1], table_pieces(ref, 0)), product(x[0] - x[1], table_pieces(ref, 1))


def synthesise(z, ref):
    even, odd = product(z[0], table_pieces(ref, 0)), product(z[1], table_pieces(ref, 1))
    return even + odd, even - odd


def circulant(x, ref):
    even, odd = analyse(x, ref)
    return even + odd, even - odd


def cut(x):
    half = x.shape[1] // 2
    return x[:, :half], x[:, half:]


def join(x):
    return jnp.concatenate(x, axis=1)


def kernel(
    x_ref, target_hbm, mobility_hbm,
    t0, t1, t2, t3, t4, t5, t6, t7,
    out_ref, residual_ref,
    v0, v1, v2, v3, v4, v5, v6, v7,
    send1, take1, send2, take2, send3, take3, send4, take4,
    turn, mine, local_part, rows_of,
    sum0, sum1, take_sum0, take_sum1, target_ref, mobility_ref,
    load_sem, send_sem, take_sem, swap_send, swap_take, sum_send, sum_take,
):
    planes, rows_local, width = x_ref.shape
    ncs = CHUNKS
    own = planes // CORES
    each = own // ncs
    vmem_tables = (v0, v1, v2, v3, v4, v5, v6, v7)
    y, x, c = (lax.axis_index(a) for a in ROW)
    chip = y * SIDE[1] + x
    other = 1 - c

    def device(p):
        return dict(zip(ROW, p, strict=True))

    def far_first(t):
        half = (t + 1) >> 1
        return 4 + half - 2 * half * (t & 1)

    def for_chips(act):
        def turn_of(k, _):
            for i in range(8):
                to_y = (y + (4, 3, 5, 2, 6, 1, 7, 0)[i]) & (SIDE[0] - 1)
                to_x = (x + far_first((k + i) & 7)) & (SIDE[1] - 1)
                if i == 7:
                    pl.when(k != 0)(functools.partial(act, to_y, to_x))
                else:
                    act(to_y, to_x)
            return 0

        lax.fori_loop(0, 8, turn_of, 0)

    first_loads = [
        pltpu.make_async_copy(a, b, load_sem.at[i])
        for i, (a, b) in enumerate(((x_ref, mine), (mobility_hbm, mobility_ref), (target_hbm, target_ref)))
    ]
    loads = [
        pltpu.make_async_copy(h, v, load_sem.at[3 + i])
        for i, (h, v) in enumerate(zip((t0, t1, t2, t3, t4, t5, t6, t7), vmem_tables, strict=True))
    ]
    for load in (first_loads[0], loads[0], *first_loads[1:]):
        load.start()

    barrier = pltpu.get_barrier_semaphore()

    def greet(to_y, to_x):
        for core in range(CORES):
            pl.semaphore_signal(barrier, inc=1, device_id=device((to_y, to_x, core)), device_id_type=MESH)

    for_chips(greet)
    pl.semaphore_signal(barrier, inc=1, device_id=device((y, x, other)), device_id_type=MESH)
    for load in loads[1:]:
        load.start()

    def spot(core, position, deep):
        return pl.ds(pl.multiple_of((core * CHIPS + position) * deep, deep), deep)

    def copy_out(src_ref, dst_ref, n, phase, p):
        return pltpu.make_async_remote_copy(
            src_ref=src_ref, dst_ref=dst_ref, send_sem=send_sem.at[n, phase], recv_sem=take_sem.at[n, phase],
            device_id=device(p), device_id_type=MESH,
        )

    def start_to_cores(src, dst, n, phase):
        deep = src.shape[1] // CHIPS // CORES
        here = spot(c, chip, deep)

        def send_one(to_y, to_x, core):
            there = spot(core, to_y * SIDE[1] + to_x, deep)
            copy_out(src.at[n, there], dst.at[n, here], n, phase, (to_y, to_x, core)).start()

        def send(to_y, to_x):
            for core in range(CORES):
                send_one(to_y, to_x, core)

        for_chips(send)
        send_one(y, x, other)
        dst[n, here, :] = src[n, here, :]

    def start_to_chips(src, dst, n, phase):
        deep = src.shape[2] // CHIPS
        here = spot(0, chip, deep)

        def send(to_y, to_x):
            there = spot(0, to_y * SIDE[1] + to_x, deep)
            copy_out(src.at[n, :, there], dst.at[n, :, here], n, phase, (to_y, to_x, c)).start()

        for_chips(send)
        for core in range(CORES):
            dst[n, core, here, :] = src[n, core, here, :]

    def whole(src, dst, n, phase):
        if len(src.shape) == 3:
            deep = src.shape[1] // CHIPS // CORES
            at = (n, pl.ds(0, deep * (CHIPS * CORES - 1)))
        else:
            deep = src.shape[2] // CHIPS
            at = (n, slice(None), pl.ds(0, deep * (CHIPS - 1)))
        return copy_out(src.at[at], dst.at[at], n, phase, (y, x, other))

    def part(ref, n, core):
        if len(ref.shape) == 3:
            rows = ref.shape[1] // CORES
            return ref.at[n, pl.ds(core * rows, rows)], rows // CHIPS
        return ref.at[n, core], ref.shape[2] // CHIPS

    def swap(n):
        return pltpu.make_async_remote_copy(
            src_ref=mine.at[pl.ds(other * own + n * each, each)],
            dst_ref=rows_of.at[n, c],
            send_sem=swap_send.at[n],
            recv_sem=swap_take.at[n],
            device_id=device((y, x, other)),
            device_id_type=MESH,
        )

    def pack_rows(fields, dst, n, core):
        dst, _ = part(dst, n, core)
        shares = 16 // len(fields) // each
        wide = width // shares
        some = min(wide, LANES)
        for j in range(0, wide, some):
            block = [f[:, s * wide + j : s * wide + j + some] for f in fields for s in range(shares)]
            dst[j : j + some, :] = jnp.concatenate(block, axis=0).T

    def unpack_rows(src, n, count):
        shares = 16 // count // each
        wide = width // shares
        rows = each * rows_local
        out = [[] for _ in range(count)]
        for core in range(CORES):
            ref, _ = part(src, n, core)
            some = min(wide, LANES)
            got = [ref[j : j + some, :].T for j in range(0, wide, some)]
            for f in range(count):
                pieces = [g[(f * shares + s) * rows : (f * shares + s + 1) * rows] for s in range(shares) for g in got]
                out[f].append(jnp.concatenate(pieces, axis=1))
        return [jnp.concatenate(o, axis=0) for o in out]

    some = CHIPS // 2

    def low_half(rows):
        return lax.broadcasted_iota(jnp.int32, (rows, LANES), 1) < LANES // 2

    def unpack_columns(src, n, count):
        refs = [part(src, n, core) for core in range(CORES)]
        deep = refs[0][1]
        for s in range(deep):
            got = [
                ref[pl.ds(s + hi * some * deep, some, stride=deep), :] for hi in range(2) for ref, _ in refs
            ]
            turn[s * LANES : (s + 1) * LANES, :] = jnp.concatenate(got, axis=0).T
        out = [([], []) for _ in range(count)]
        low = low_half(deep * 16 // count)
        for a in range(0, rows_local, 2):
            pair = [
                turn[pl.ds(a + i, deep * 16, stride=rows_local), :].reshape(deep, count, 16 // count, LANES)
                for i in range(2)
            ]
            for f in range(count):
                one, two = (g[:, f].reshape(deep * 16 // count, LANES) for g in pair)
                out[f][0].append(jnp.where(low, one, pltpu.roll(two, LANES // 2, 1)))
                out[f][1].append(jnp.where(low, pltpu.roll(one, LANES // 2, 1), two))
        return [tuple(jnp.concatenate(h, axis=1) for h in o) for o in out]

    def pack_columns(fields, dst, n):
        count = len(fields)
        refs = [part(dst, n, core) for core in range(CORES)]
        deep = refs[0][1]
        low = low_half(deep * 16 // count)
        for a in range(0, rows_local, 2):
            at = slice(a // 2 * LANES, (a // 2 + 1) * LANES)
            pair = ([], [])
            for f in fields:
                near, far = f[0][:, at], f[1][:, at]
                pair[0].append(jnp.where(low, near, pltpu.roll(far, LANES // 2, 1)))
                pair[1].append(jnp.where(low, pltpu.roll(near, LANES // 2, 1), far))
            for i in range(2):
                got = [g.reshape(deep, 1, 16 // count, LANES) for g in pair[i]]
                turn[pl.ds(a + i, deep * 16, stride=rows_local), :] = jnp.concatenate(got, axis=1).reshape(
                    deep * 16, LANES
                )
        for s in range(deep):
            both = turn[s * LANES : (s + 1) * LANES, :].T
            for hi in range(2):
                for core, (ref, _) in enumerate(refs):
                    at = (hi * CORES + core) * some
                    ref[pl.ds(s + hi * some * deep, some, stride=deep), :] = both[at : at + some]

    def per_plane(shape, plane_of_row, n):
        out = jnp.zeros(shape, jnp.float32)
        for p in range(each):
            out = jnp.where(plane_of_row == p, mobility_ref[c * own + n * each + p], out)
        return out

    waited = set()

    def table(i):
        if i not in waited:
            waited.add(i)
            loads[i].wait()
        return vmem_tables[i]

    def start_fields():
        first_loads[0].wait()
        field = mine[...].reshape(planes * rows_local, width)
        local = field * field * field - field + stiffness * join(circulant(cut(field), table(0)))
        local_part[...] = local.reshape(planes, rows_local, width)
        for n in range(ncs):
            for core in range(CORES):
                at = slice(core * own + n * each, core * own + (n + 1) * each)
                fields = [ref[at].reshape(each * rows_local, width) for ref in (mine, local_part)]
                pack_rows(fields, send1, n, core)

    def columns_middle(n):
        field, local = unpack_columns(take1, n, 2)
        potential = [u + stiffness * v for u, v in zip(local, circulant(field, table(1)), strict=True)]
        slope = circulant(potential, table(2))
        rows = lax.broadcasted_iota(jnp.int32, (field[0].shape[0], LANES), 0)
        scale = per_plane(rows.shape, rows % each, n)
        scale = jnp.concatenate([scale] * (field[0].shape[1] // LANES), axis=1)
        flux = [scale / (1.0 + f * f) * g for f, g in zip(field, slope, strict=True)]
        pack_columns([potential, circulant(flux, table(2))], send2, n)

    def row_weight(n):
        for p in range(each):
            rows_of[n, c, p] = mine[c * own + n * each + p]
        swap(n).wait_recv()
        field = rows_of[n].reshape(CORES * each * rows_local, width)
        rows = lax.broadcasted_iota(jnp.int32, (field.shape[0], LANES), 0)
        scale = per_plane(rows.shape, rows // rows_local % each, n)
        scale = jnp.concatenate([scale] * (width // LANES), axis=1)
        rows_of[n] = (scale / (1.0 + field * field)).reshape(rows_of.shape[1:])

    def rows_middle(n):
        potential, spread = unpack_rows(take2, n, 2)
        slope = join(circulant(cut(potential), table(3)))
        weight = rows_of[n].reshape(slope.shape)
        total = spread + join(circulant(cut(weight * slope), table(3)))
        spectrum = join(analyse(cut(total), table(4)))
        rows = each * rows_local
        for core in range(CORES):
            pack_rows([spectrum[core * rows : (core + 1) * rows]], send3, n, core)

    def columns_solve(n):
        deep = take3.shape[2] // CHIPS
        shares = 16 // each
        rows = lax.broadcasted_iota(jnp.int32, (deep * 16, LANES), 0)
        slot_y = rows % 16 // each * (width // shares) + chip * deep + rows // 16
        scale = per_plane(rows.shape, rows % each, n)
        step = 2.0 * math.pi / width
        wave_y = slots(slot_y, width)[0].astype(jnp.float32) * step
        length = CHIPS * CORES * rows_local
        slot_x = lax.broadcasted_iota(jnp.int32, (8, length), 1)
        wave_x = slots(slot_x, length)[0].astype(jnp.float32) * (2.0 * math.pi / length)
        square_x = (wave_x * wave_x)[:1]
        wide = length // LANES
        square = jnp.concatenate([wave_y * wave_y] * wide, axis=1) + square_x
        denom = 1.0 + time_step * jnp.concatenate([scale] * wide, axis=1) * (
            stabilizer * square + stiffness * square * square
        )
        factor = time_step / denom
        whole(send3, take3, n, 2).wait_recv()
        (spectrum,) = unpack_columns(take3, n, 1)
        solved = [z * f for z, f in zip(analyse(spectrum, table(5)), cut(factor), strict=True)]
        pack_columns([synthesise(solved, table(6))], send4, n)

    def residual():
        total = jnp.sum(take_sum1[...], axis=0)
        length = CHIPS * CORES * rows_local
        mean = jnp.sum(total, axis=1, keepdims=True) * (1.0 / (length * width))
        row = lax.broadcasted_iota(jnp.int32, (planes, LANES), 0)
        first_loads[2].wait()
        target = jnp.zeros((planes, LANES), jnp.float32)
        for p in range(planes):
            target = jnp.where(row == p, target_ref[p], target)
        residual_ref[...] = mean - target

    def rows_end(n):
        (spectrum,) = unpack_rows(take4, n, 1)
        change = join(synthesise(cut(spectrum), table(7))).reshape(CORES, each, rows_local, width)
        for core in range(CORES):
            at = slice(core * own + n * each, core * own + (n + 1) * each)
            down = jnp.concatenate([residual_ref[at][:, None, :]] * (width // LANES), axis=2)
            out_ref[at] = mine[at] + change[core] - down

    sums = ((sum0, take_sum0), (sum1, take_sum1))
    near = [(0, dx, dc) for dx in range(SIDE[1]) for dc in range(SIDE[2])][1:]
    across = [(dy, 0, 0) for dy in range(1, SIDE[0])]

    def place(dy, dx, dc):
        return (y + dy) & (SIDE[0] - 1), (x + dx) & (SIDE[1] - 1), (c + dc) & (SIDE[2] - 1)

    def sum_slot(stage, p):
        return p[0] if stage else p[1] * SIDE[2] + p[2]

    def sum_copy(stage, index, p, sender):
        src, dst = sums[stage]
        slot = sum_slot(stage, sender)
        return pltpu.make_async_remote_copy(
            src_ref=src, dst_ref=dst.at[slot], send_sem=sum_send.at[stage, index], recv_sem=sum_take.at[stage, slot],
            device_id=device(p), device_id_type=MESH,
        )

    def start_sums(stage, places):
        for i, d in enumerate(places):
            sum_copy(stage, i, place(*d), (y, x, c)).start()
        src, dst = sums[stage]
        dst[sum_slot(stage, (y, x, c))] = src[...]

    def take_sums(stage, places):
        for i, d in enumerate(places):
            sum_copy(stage, i, (y, x, other), place(*d)).wait_recv()

    start_fields()
    summed = jnp.sum(mine[...], axis=1)
    partial = summed[:, :LANES]
    for j in range(1, width // LANES):
        partial = partial + summed[:, j * LANES : (j + 1) * LANES]
    sum0[...] = partial

    pl.semaphore_wait(barrier, CHIPS * CORES - 1)
    for n in range(ncs):
        start_to_cores(send1, take1, n, 0)
    start_sums(0, near)
    for n in range(ncs):
        swap(n).start()
    first_loads[1].wait()
    for n in range(ncs):
        row_weight(n)
    for n in range(ncs):
        whole(send1, take1, n, 0).wait_recv()
        columns_middle(n)
        start_to_chips(send2, take2, n, 1)
    take_sums(0, near)
    sum1[...] = jnp.sum(take_sum0[...], axis=0)
    start_sums(1, across)
    for n in range(ncs):
        whole(send2, take2, n, 1).wait_recv()
        rows_middle(n)
        start_to_chips(send3, take3, n, 2)
    for n in range(ncs):
        columns_solve(n)
        start_to_cores(send4, take4, n, 3)
    take_sums(1, across)
    residual()
    for n in range(ncs):
        whole(send4, take4, n, 3).wait_recv()
        rows_end(n)
    for n in range(ncs):
        for phase, (src, dst) in enumerate(((send1, take1), (send2, take2), (send3, take3), (send4, take4))):
            whole(src, dst, n, phase).wait_send()
        swap(n).wait_send()
    for stage, places in enumerate((near, across)):
        for i, d in enumerate(places):
            sum_copy(stage, i, place(*d), (y, x, c)).wait_send()


def hand_over(updated_ref, residual_ref, out_ref, out_residual_ref):
    out_ref[...] = updated_ref[...]
    for p in range(out_residual_ref.shape[0]):
        out_residual_ref[p] = residual_ref[p, 0]


def local(concentration, target_mass, mobility):
    planes, rows_local, width = concentration.shape
    data = tables(width)
    ncs = CHUNKS
    each = planes // CORES // ncs
    rows = CHIPS * CORES * each
    shape = {1: (ncs, 2 * rows, LANES), 2: (ncs, CORES, rows, LANES), 3: (ncs, CORES, rows // 2, LANES), 4: (ncs, rows, LANES)}
    vmem = pl.BlockSpec(memory_space=pltpu.VMEM)
    updated, residual = pl.pallas_call(
        kernel,
        out_shape=(
            jax.ShapeDtypeStruct(concentration.shape, jnp.float32),
            jax.ShapeDtypeStruct((planes, LANES), jnp.float32),
        ),
        in_specs=[pl.BlockSpec(memory_space=pl.ANY)] * (3 + len(data)),
        out_specs=(vmem, vmem),
        scratch_shapes=[pltpu.VMEM(t.shape, jnp.bfloat16) for t in data]
        + [pltpu.VMEM(shape[phase], jnp.float32) for phase in (1, 2, 3, 4) for _ in range(2)]
        + [
            pltpu.VMEM((2 * rows, LANES), jnp.float32),
            pltpu.VMEM((planes, rows_local, width), jnp.float32),
            pltpu.VMEM((planes, rows_local, width), jnp.float32),
            pltpu.VMEM((ncs, CORES, each, rows_local, width), jnp.float32),
            pltpu.VMEM((planes, LANES), jnp.float32),
            pltpu.VMEM((planes, LANES), jnp.float32),
            pltpu.VMEM((SIDE[1] * SIDE[2], planes, LANES), jnp.float32),
            pltpu.VMEM((SIDE[0], planes, LANES), jnp.float32),
            pltpu.SMEM((planes,), jnp.float32),
            pltpu.SMEM((planes,), jnp.float32),
            pltpu.SemaphoreType.DMA((3 + len(data),)),
            pltpu.SemaphoreType.DMA((ncs, 4)),
            pltpu.SemaphoreType.DMA((ncs, 4)),
            pltpu.SemaphoreType.DMA((ncs,)),
            pltpu.SemaphoreType.DMA((ncs,)),
            pltpu.SemaphoreType.DMA((2, SIDE[1] * SIDE[2])),
            pltpu.SemaphoreType.DMA((2, SIDE[1] * SIDE[2])),
        ],
        compiler_params=pltpu.CompilerParams(
            collective_id=0, has_side_effects=True, vmem_limit_bytes=60 * 2**20
        ),
    )(concentration, target_mass, mobility, *[jnp.asarray(t) for t in data])
    smem = pl.BlockSpec(memory_space=pltpu.SMEM)
    return pl.pallas_call(
        hand_over,
        out_shape=(
            jax.ShapeDtypeStruct(concentration.shape, jnp.float32),
            jax.ShapeDtypeStruct((planes,), jnp.float32),
        ),
        in_specs=[vmem, smem],
        out_specs=(vmem, smem),
    )(updated, residual)


def solution(mesh):
    torus = Mesh(mesh.devices.reshape(mesh.shape["grp"], *SIDE), ("grp", *ROW))
    in_specs = (P("grp", ROW, None), P("grp"), P("grp"))
    out_specs = (P("grp", ROW, None), P("grp"))
    return jax.shard_map(local, mesh=torus, in_specs=in_specs, out_specs=out_specs, check_vma=False)
```

```python
import functools
import math

import jax
import jax.numpy as jnp
import ml_dtypes
import numpy as np
from jax import lax
from jax.experimental import pallas as pl
from jax.experimental.pallas import tpu as pltpu
from jax.sharding import Mesh
from jax.sharding import PartitionSpec as P

ROW = ("row_0", "row_1", "row_2")
MESH = pl.DeviceIdType.MESH
SIDE = (8, 8, 2)
CHIPS = SIDE[0] * SIDE[1]
CORES = SIDE[2]
LANES = 128
CHUNKS = 2

stiffness = 1.0
time_step = 0.05
stabilizer = 2.0


def split(table):
    high = table.astype(ml_dtypes.bfloat16)
    low = (table - high.astype(np.float64)).astype(ml_dtypes.bfloat16)
    return np.stack([high, low])


def circulants(length):
    position = np.arange(length)
    signed = np.where(position < length // 2, position, position - length)
    angular = signed * (2.0 * math.pi / length)
    derivative = np.where(position == length // 2, 0.0, angular)
    offset = (position[None, :] - position[:, None]) % length
    second = np.fft.ifft(angular**2).real[offset]
    first = np.fft.ifft(1j * derivative).real[offset]
    return second, first


def real_basis(length):
    wave, is_sine = slots(np.arange(length), length)
    angle = np.outer(np.arange(length), wave) % length * (2.0 * math.pi / length)
    plain = (wave == 0) | (wave == length // 2)
    scale = np.where(plain, np.sqrt(1.0 / length), np.sqrt(2.0 / length))
    return np.where(is_sine & ~plain, np.sin(angle), np.cos(angle)) * scale


def slots(slot, length):
    quarter = length // 4
    odd = slot // (2 * quarter)
    within = slot % (2 * quarter)
    is_sine = within // quarter
    wave = 2 * (within % quarter) + odd
    nyquist = (is_sine == 1) & (wave == 0)
    if isinstance(slot, np.ndarray):
        return np.where(nyquist, length // 2, wave), is_sine == 1
    return jnp.where(nyquist, length // 2, wave), is_sine == 1


def halves(matrix, order):
    half = matrix.shape[0] // 2
    near, far = matrix[order][:, order], matrix[order][:, order + half]
    return np.stack([near + far, near - far]) / 2


@functools.cache
def tables(length):
    second, first = circulants(length)
    basis = real_basis(length)
    half = length // 2
    rows = np.arange(half)
    columns = rows.reshape(CHIPS // 2, CORES, -1).transpose(2, 1, 0).reshape(-1)
    row_basis, column_basis = (np.stack([basis[o][:, :half], basis[o][:, half:]]) for o in (rows, columns))
    return tuple(
        split(t)
        for t in (
            halves(second, rows),
            halves(second, columns),
            halves(first, columns),
            halves(first, rows),
            row_basis,
            column_basis,
            np.swapaxes(column_basis, 1, 2),
            np.swapaxes(row_basis, 1, 2),
        )
    )


def parts(x):
    high = x.astype(jnp.bfloat16)
    low = (x - high.astype(jnp.float32)).astype(jnp.bfloat16)
    return high, jnp.concatenate([high, low], axis=0)


def product(x, pieces):
    m = x.shape[0]
    high, both = parts(x)
    inputs, outputs, piece = pieces
    out = []
    for j in range(outputs):
        total = None
        for i in range(inputs):
            at = slice(i * 256, (i + 1) * 256)
            wide = jnp.dot(both[:, at], piece(i, j, 0), preferred_element_type=jnp.float32)
            narrow = jnp.dot(high[:, at], piece(i, j, 1), preferred_element_type=jnp.float32)
            term = (wide, narrow)
            total = term if total is None else (total[0] + wide, total[1] + narrow)
        out.append(total[0][:m] + total[0][m:] + total[1])
    return jnp.concatenate(out, axis=1)


def table_pieces(ref, which):
    n = ref.shape[2] // 256
    return n, n, lambda i, j, part: ref[part, which, i * 256 : (i + 1) * 256, j * 256 : (j + 1) * 256]


def analyse(x, ref):
    return product(x[0] + x[1], table_pieces(ref, 0)), product(x[0] - x[1], table_pieces(ref, 1))


def synthesise(z, ref):
    even, odd = product(z[0], table_pieces(ref, 0)), product(z[1], table_pieces(ref, 1))
    return even + odd, even - odd


def circulant(x, ref):
    even, odd = analyse(x, ref)
    return even + odd, even - odd


def cut(x):
    half = x.shape[1] // 2
    return x[:, :half], x[:, half:]


def join(x):
    return jnp.concatenate(x, axis=1)


def far_first():
    groups = {}
    for dy in range(SIDE[0]):
        for dx in range(SIDE[1]):
            far = min(dy, SIDE[0] - dy) + min(dx, SIDE[1] - dx)
            way = (2 * dy > SIDE[0], 2 * dx > SIDE[1])
            if far:
                groups.setdefault(far, {}).setdefault(way, []).append((dy, dx))
    out = []
    for far in sorted(groups, reverse=True):
        ways = [groups[far][w] for w in ((0, 0), (1, 1), (0, 1), (1, 0)) if w in groups[far]]
        for turn in range(max(map(len, ways))):
            out += [w[turn] for w in ways if turn < len(w)]
    return out


def kernel(
    x_ref, target_hbm, mobility_hbm,
    t0, t1, t2, t3, t4, t5, t6, t7,
    out_ref, residual_ref,
    v0, v1, v2, v3, v4, v5, v6, v7,
    send1, take1, send2, take2, send3, take3, send4, take4,
    turn, mine, local_part, rows_of,
    sum0, sum1, take_sum0, take_sum1, target_ref, mobility_ref,
    load_sem, send_sem, take_sem, swap_send, swap_take, sum_send, sum_take,
):
    planes, rows_local, width = x_ref.shape
    ncs = CHUNKS
    own = planes // CORES
    each = own // ncs
    vmem_tables = (v0, v1, v2, v3, v4, v5, v6, v7)
    y, x, c = (lax.axis_index(a) for a in ROW)
    chip = y * SIDE[1] + x
    other = 1 - c

    def device(p):
        return dict(zip(ROW, p, strict=True))

    def for_chips(act):
        for dy, dx in far_first():
            act((y + dy) & (SIDE[0] - 1), (x + dx) & (SIDE[1] - 1))

    first_loads = [
        pltpu.make_async_copy(a, b, load_sem.at[i])
        for i, (a, b) in enumerate(((x_ref, mine), (mobility_hbm, mobility_ref), (target_hbm, target_ref)))
    ]
    loads = [
        pltpu.make_async_copy(h, v, load_sem.at[3 + i])
        for i, (h, v) in enumerate(zip((t0, t1, t2, t3, t4, t5, t6, t7), vmem_tables, strict=True))
    ]
    for load in (first_loads[0], loads[0], *first_loads[1:]):
        load.start()

    barrier = pltpu.get_barrier_semaphore()

    def greet(to_y, to_x):
        for core in range(CORES):
            pl.semaphore_signal(barrier, inc=1, device_id=device((to_y, to_x, core)), device_id_type=MESH)

    for_chips(greet)
    pl.semaphore_signal(barrier, inc=1, device_id=device((y, x, other)), device_id_type=MESH)
    for load in loads[1:]:
        load.start()

    def spot(core, position, deep):
        return pl.ds(pl.multiple_of((core * CHIPS + position) * deep, deep), deep)

    def copy_out(src_ref, dst_ref, n, phase, p):
        return pltpu.make_async_remote_copy(
            src_ref=src_ref, dst_ref=dst_ref, send_sem=send_sem.at[n, phase], recv_sem=take_sem.at[n, phase],
            device_id=device(p), device_id_type=MESH,
        )

    def start_to_cores(src, dst, n, phase):
        deep = src.shape[1] // CHIPS // CORES
        here = spot(c, chip, deep)

        def send_one(to_y, to_x, core):
            there = spot(core, to_y * SIDE[1] + to_x, deep)
            copy_out(src.at[n, there], dst.at[n, here], n, phase, (to_y, to_x, core)).start()

        def send(to_y, to_x):
            for core in range(CORES):
                send_one(to_y, to_x, core)

        for_chips(send)
        send_one(y, x, other)
        dst[n, here, :] = src[n, here, :]

    def start_to_chips(src, dst, n, phase):
        deep = src.shape[2] // CHIPS
        here = spot(0, chip, deep)

        def send(to_y, to_x):
            there = spot(0, to_y * SIDE[1] + to_x, deep)
            copy_out(src.at[n, :, there], dst.at[n, :, here], n, phase, (to_y, to_x, c)).start()

        for_chips(send)
        for core in range(CORES):
            dst[n, core, here, :] = src[n, core, here, :]

    def whole(src, dst, n, phase):
        if len(src.shape) == 3:
            deep = src.shape[1] // CHIPS // CORES
            at = (n, pl.ds(0, deep * (CHIPS * CORES - 1)))
        else:
            deep = src.shape[2] // CHIPS
            at = (n, slice(None), pl.ds(0, deep * (CHIPS - 1)))
        return copy_out(src.at[at], dst.at[at], n, phase, (y, x, other))

    def part(ref, n, core):
        if len(ref.shape) == 3:
            rows = ref.shape[1] // CORES
            return ref.at[n, pl.ds(core * rows, rows)], rows // CHIPS
        return ref.at[n, core], ref.shape[2] // CHIPS

    def swap(n):
        return pltpu.make_async_remote_copy(
            src_ref=mine.at[pl.ds(other * own + n * each, each)],
            dst_ref=rows_of.at[n, c],
            send_sem=swap_send.at[n],
            recv_sem=swap_take.at[n],
            device_id=device((y, x, other)),
            device_id_type=MESH,
        )

    def pack_rows(fields, dst, n, core):
        dst, _ = part(dst, n, core)
        shares = 16 // len(fields) // each
        wide = width // shares
        some = min(wide, LANES)
        for j in range(0, wide, some):
            block = [f[:, s * wide + j : s * wide + j + some] for f in fields for s in range(shares)]
            dst[j : j + some, :] = jnp.concatenate(block, axis=0).T

    def unpack_rows(src, n, count):
        shares = 16 // count // each
        wide = width // shares
        rows = each * rows_local
        out = [[] for _ in range(count)]
        for core in range(CORES):
            ref, _ = part(src, n, core)
            some = min(wide, LANES)
            got = [ref[j : j + some, :].T for j in range(0, wide, some)]
            for f in range(count):
                pieces = [g[(f * shares + s) * rows : (f * shares + s + 1) * rows] for s in range(shares) for g in got]
                out[f].append(jnp.concatenate(pieces, axis=1))
        return [jnp.concatenate(o, axis=0) for o in out]

    some = CHIPS // 2

    def low_half(rows):
        return lax.broadcasted_iota(jnp.int32, (rows, LANES), 1) < LANES // 2

    def unpack_columns(src, n, count):
        refs = [part(src, n, core) for core in range(CORES)]
        deep = refs[0][1]
        for s in range(deep):
            got = [
                ref[pl.ds(s + hi * some * deep, some, stride=deep), :] for hi in range(2) for ref, _ in refs
            ]
            turn[s * LANES : (s + 1) * LANES, :] = jnp.concatenate(got, axis=0).T
        out = [([], []) for _ in range(count)]
        low = low_half(deep * 16 // count)
        for a in range(0, rows_local, 2):
            pair = [
                turn[pl.ds(a + i, deep * 16, stride=rows_local), :].reshape(deep, count, 16 // count, LANES)
                for i in range(2)
            ]
            for f in range(count):
                one, two = (g[:, f].reshape(deep * 16 // count, LANES) for g in pair)
                out[f][0].append(jnp.where(low, one, pltpu.roll(two, LANES // 2, 1)))
                out[f][1].append(jnp.where(low, pltpu.roll(one, LANES // 2, 1), two))
        return [tuple(jnp.concatenate(h, axis=1) for h in o) for o in out]

    def pack_columns(fields, dst, n):
        count = len(fields)
        refs = [part(dst, n, core) for core in range(CORES)]
        deep = refs[0][1]
        low = low_half(deep * 16 // count)
        for a in range(0, rows_local, 2):
            at = slice(a // 2 * LANES, (a // 2 + 1) * LANES)
            pair = ([], [])
            for f in fields:
                near, far = f[0][:, at], f[1][:, at]
                pair[0].append(jnp.where(low, near, pltpu.roll(far, LANES // 2, 1)))
                pair[1].append(jnp.where(low, pltpu.roll(near, LANES // 2, 1), far))
            for i in range(2):
                got = [g.reshape(deep, 1, 16 // count, LANES) for g in pair[i]]
                turn[pl.ds(a + i, deep * 16, stride=rows_local), :] = jnp.concatenate(got, axis=1).reshape(
                    deep * 16, LANES
                )
        for s in range(deep):
            both = turn[s * LANES : (s + 1) * LANES, :].T
            for hi in range(2):
                for core, (ref, _) in enumerate(refs):
                    at = (hi * CORES + core) * some
                    ref[pl.ds(s + hi * some * deep, some, stride=deep), :] = both[at : at + some]

    def per_plane(shape, plane_of_row, n):
        out = jnp.zeros(shape, jnp.float32)
        for p in range(each):
            out = jnp.where(plane_of_row == p, mobility_ref[c * own + n * each + p], out)
        return out

    waited = set()

    def table(i):
        if i not in waited:
            waited.add(i)
            loads[i].wait()
        return vmem_tables[i]

    def start_fields():
        first_loads[0].wait()
        field = mine[...].reshape(planes * rows_local, width)
        local = field * field * field - field + stiffness * join(circulant(cut(field), table(0)))
        local_part[...] = local.reshape(planes, rows_local, width)
        for n in range(ncs):
            for core in range(CORES):
                at = slice(core * own + n * each, core * own + (n + 1) * each)
                fields = [ref[at].reshape(each * rows_local, width) for ref in (mine, local_part)]
                pack_rows(fields, send1, n, core)

    def columns_middle(n):
        field, local = unpack_columns(take1, n, 2)
        potential = [u + stiffness * v for u, v in zip(local, circulant(field, table(1)), strict=True)]
        slope = circulant(potential, table(2))
        rows = lax.broadcasted_iota(jnp.int32, (field[0].shape[0], LANES), 0)
        scale = per_plane(rows.shape, rows % each, n)
        scale = jnp.concatenate([scale] * (field[0].shape[1] // LANES), axis=1)
        flux = [scale / (1.0 + f * f) * g for f, g in zip(field, slope, strict=True)]
        pack_columns([potential, circulant(flux, table(2))], send2, n)

    def row_weight(n):
        for p in range(each):
            rows_of[n, c, p] = mine[c * own + n * each + p]
        swap(n).wait_recv()
        field = rows_of[n].reshape(CORES * each * rows_local, width)
        rows = lax.broadcasted_iota(jnp.int32, (field.shape[0], LANES), 0)
        scale = per_plane(rows.shape, rows // rows_local % each, n)
        scale = jnp.concatenate([scale] * (width // LANES), axis=1)
        rows_of[n] = (scale / (1.0 + field * field)).reshape(rows_of.shape[1:])

    def rows_middle(n):
        potential, spread = unpack_rows(take2, n, 2)
        slope = join(circulant(cut(potential), table(3)))
        weight = rows_of[n].reshape(slope.shape)
        both = jnp.concatenate([weight * slope, spread], axis=0)
        count = slope.shape[0]
        quarter = width // 4
        place_of = lax.broadcasted_iota(jnp.int32, (8, quarter), 1)[:1]
        spectrum = []
        for odd, z in enumerate(analyse(cut(both), table(4))):
            wave = (2 * place_of + odd).astype(jnp.float32) * (2.0 * math.pi / width)
            cosine, sine = z[:count, :quarter], z[:count, quarter:]
            spectrum += [z[count:, :quarter] + wave * sine, z[count:, quarter:] - wave * cosine]
        spectrum = join(spectrum)
        rows = each * rows_local
        for core in range(CORES):
            pack_rows([spectrum[core * rows : (core + 1) * rows]], send3, n, core)

    def columns_solve(n):
        deep = take3.shape[2] // CHIPS
        shares = 16 // each
        rows = lax.broadcasted_iota(jnp.int32, (deep * 16, LANES), 0)
        slot_y = rows % 16 // each * (width // shares) + chip * deep + rows // 16
        scale = per_plane(rows.shape, rows % each, n)
        step = 2.0 * math.pi / width
        wave_y = slots(slot_y, width)[0].astype(jnp.float32) * step
        length = CHIPS * CORES * rows_local
        slot_x = lax.broadcasted_iota(jnp.int32, (8, length), 1)
        wave_x = slots(slot_x, length)[0].astype(jnp.float32) * (2.0 * math.pi / length)
        square_x = (wave_x * wave_x)[:1]
        wide = length // LANES
        square = jnp.concatenate([wave_y * wave_y] * wide, axis=1) + square_x
        denom = 1.0 + time_step * jnp.concatenate([scale] * wide, axis=1) * (
            stabilizer * square + stiffness * square * square
        )
        factor = time_step / denom
        whole(send3, take3, n, 2).wait_recv()
        (spectrum,) = unpack_columns(take3, n, 1)
        solved = [z * f for z, f in zip(analyse(spectrum, table(5)), cut(factor), strict=True)]
        pack_columns([synthesise(solved, table(6))], send4, n)

    def residual():
        total = jnp.sum(take_sum1[...], axis=0)
        length = CHIPS * CORES * rows_local
        mean = jnp.sum(total, axis=1, keepdims=True) * (1.0 / (length * width))
        row = lax.broadcasted_iota(jnp.int32, (planes, LANES), 0)
        first_loads[2].wait()
        target = jnp.zeros((planes, LANES), jnp.float32)
        for p in range(planes):
            target = jnp.where(row == p, target_ref[p], target)
        residual_ref[...] = mean - target

    def rows_end(n):
        (spectrum,) = unpack_rows(take4, n, 1)
        change = join(synthesise(cut(spectrum), table(7))).reshape(CORES, each, rows_local, width)
        for core in range(CORES):
            at = slice(core * own + n * each, core * own + (n + 1) * each)
            down = jnp.concatenate([residual_ref[at][:, None, :]] * (width // LANES), axis=2)
            out_ref[at] = mine[at] + change[core] - down

    sums = ((sum0, take_sum0), (sum1, take_sum1))
    near = [(0, dx, dc) for dx in range(SIDE[1]) for dc in range(SIDE[2])][1:]
    across = [(dy, 0, 0) for dy in range(1, SIDE[0])]

    def place(dy, dx, dc):
        return (y + dy) & (SIDE[0] - 1), (x + dx) & (SIDE[1] - 1), (c + dc) & (SIDE[2] - 1)

    def sum_slot(stage, p):
        return p[0] if stage else p[1] * SIDE[2] + p[2]

    def sum_copy(stage, index, p, sender):
        src, dst = sums[stage]
        slot = sum_slot(stage, sender)
        return pltpu.make_async_remote_copy(
            src_ref=src, dst_ref=dst.at[slot], send_sem=sum_send.at[stage, index], recv_sem=sum_take.at[stage, slot],
            device_id=device(p), device_id_type=MESH,
        )

    def start_sums(stage, places):
        for i, d in enumerate(places):
            sum_copy(stage, i, place(*d), (y, x, c)).start()
        src, dst = sums[stage]
        dst[sum_slot(stage, (y, x, c))] = src[...]

    def take_sums(stage, places):
        for i, d in enumerate(places):
            sum_copy(stage, i, (y, x, other), place(*d)).wait_recv()

    start_fields()
    summed = jnp.sum(mine[...], axis=1)
    partial = summed[:, :LANES]
    for j in range(1, width // LANES):
        partial = partial + summed[:, j * LANES : (j + 1) * LANES]
    sum0[...] = partial

    pl.semaphore_wait(barrier, CHIPS * CORES - 1)
    for n in range(ncs):
        start_to_cores(send1, take1, n, 0)
    start_sums(0, near)
    for n in range(ncs):
        swap(n).start()
    first_loads[1].wait()
    for n in range(ncs):
        row_weight(n)
    for n in range(ncs):
        whole(send1, take1, n, 0).wait_recv()
        columns_middle(n)
        start_to_chips(send2, take2, n, 1)
    take_sums(0, near)
    sum1[...] = jnp.sum(take_sum0[...], axis=0)
    start_sums(1, across)
    for n in range(ncs):
        whole(send2, take2, n, 1).wait_recv()
        rows_middle(n)
        start_to_chips(send3, take3, n, 2)
    for n in range(ncs):
        columns_solve(n)
        start_to_cores(send4, take4, n, 3)
    take_sums(1, across)
    residual()
    for n in range(ncs):
        whole(send4, take4, n, 3).wait_recv()
        rows_end(n)
    for n in range(ncs):
        for phase, (src, dst) in enumerate(((send1, take1), (send2, take2), (send3, take3), (send4, take4))):
            whole(src, dst, n, phase).wait_send()
        swap(n).wait_send()
    for stage, places in enumerate((near, across)):
        for i, d in enumerate(places):
            sum_copy(stage, i, place(*d), (y, x, c)).wait_send()


def hand_over(updated_ref, residual_ref, out_ref, out_residual_ref):
    out_ref[...] = updated_ref[...]
    for p in range(out_residual_ref.shape[0]):
        out_residual_ref[p] = residual_ref[p, 0]


def local(concentration, target_mass, mobility):
    planes, rows_local, width = concentration.shape
    data = tables(width)
    ncs = CHUNKS
    each = planes // CORES // ncs
    rows = CHIPS * CORES * each
    shape = {1: (ncs, 2 * rows, LANES), 2: (ncs, CORES, rows, LANES), 3: (ncs, CORES, rows // 2, LANES), 4: (ncs, rows, LANES)}
    vmem = pl.BlockSpec(memory_space=pltpu.VMEM)
    updated, residual = pl.pallas_call(
        kernel,
        out_shape=(
            jax.ShapeDtypeStruct(concentration.shape, jnp.float32),
            jax.ShapeDtypeStruct((planes, LANES), jnp.float32),
        ),
        in_specs=[pl.BlockSpec(memory_space=pl.ANY)] * (3 + len(data)),
        out_specs=(vmem, vmem),
        scratch_shapes=[pltpu.VMEM(t.shape, jnp.bfloat16) for t in data]
        + [pltpu.VMEM(shape[phase], jnp.float32) for phase in (1, 2, 3, 4) for _ in range(2)]
        + [
            pltpu.VMEM((2 * rows, LANES), jnp.float32),
            pltpu.VMEM((planes, rows_local, width), jnp.float32),
            pltpu.VMEM((planes, rows_local, width), jnp.float32),
            pltpu.VMEM((ncs, CORES, each, rows_local, width), jnp.float32),
            pltpu.VMEM((planes, LANES), jnp.float32),
            pltpu.VMEM((planes, LANES), jnp.float32),
            pltpu.VMEM((SIDE[1] * SIDE[2], planes, LANES), jnp.float32),
            pltpu.VMEM((SIDE[0], planes, LANES), jnp.float32),
            pltpu.SMEM((planes,), jnp.float32),
            pltpu.SMEM((planes,), jnp.float32),
            pltpu.SemaphoreType.DMA((3 + len(data),)),
            pltpu.SemaphoreType.DMA((ncs, 4)),
            pltpu.SemaphoreType.DMA((ncs, 4)),
            pltpu.SemaphoreType.DMA((ncs,)),
            pltpu.SemaphoreType.DMA((ncs,)),
            pltpu.SemaphoreType.DMA((2, SIDE[1] * SIDE[2])),
            pltpu.SemaphoreType.DMA((2, SIDE[1] * SIDE[2])),
        ],
        compiler_params=pltpu.CompilerParams(
            collective_id=0, has_side_effects=True, vmem_limit_bytes=60 * 2**20
        ),
    )(concentration, target_mass, mobility, *[jnp.asarray(t) for t in data])
    smem = pl.BlockSpec(memory_space=pltpu.SMEM)
    return pl.pallas_call(
        hand_over,
        out_shape=(
            jax.ShapeDtypeStruct(concentration.shape, jnp.float32),
            jax.ShapeDtypeStruct((planes,), jnp.float32),
        ),
        in_specs=[vmem, smem],
        out_specs=(vmem, smem),
    )(updated, residual)


def solution(mesh):
    torus = Mesh(mesh.devices.reshape(mesh.shape["grp"], *SIDE), ("grp", *ROW))
    in_specs = (P("grp", ROW, None), P("grp"), P("grp"))
    out_specs = (P("grp", ROW, None), P("grp"))
    return jax.shard_map(local, mesh=torus, in_specs=in_specs, out_specs=out_specs, check_vma=False)
```
